32 devices in a mesh: group: 4 (over x, core), shard: 8 (over z, y).
Axes of the slice: x: 2, y: 2, z: 4, core: 2. Of those that a mesh axis runs over, the one named last changes fastest.
Arguments:
- step_index: int32 [1], replicated, may hold values from 0 to 1023
- hidden: bfloat16 [4, 8192, 4608], P('group', 'shard'), may hold values from -600 to 600
- upstream: bfloat16 [4, 8192, 2304], P('group', 'shard'), may hold values from -40 to 40
- numerator: float32 [4, 4608, 2304], P('group', 'shard'), may hold values from -6 to 6
- push_weight: float32 [4], P('group'), may hold values from 0.5 to 2
Outputs:
- numerator_next: float32 [4, 4608, 2304], P('group', 'shard')
- weight_next: float32 [4], P('group')
- params: bfloat16 [4, 4608, 2304], P('group', 'shard')
The draws below stay inside these ranges and needn't reach their ends.
All inputs are finite; a program needn't handle non-finite values.
Results may differ from the reference program's by a relative error of at most 0.009.
Values may be sent and summed in bfloat16 or wider, within the bound.
A program may use at most 128 MiB of HBM per device.

```python
import math
import jax
import jax.numpy as jnp
from jax import lax

D = 2304
FF = 4608
TOK_DEV = 1024
GROUPS = 4
SHARDS = 8
TOK_GROUP = 8192


def draw_hidden(key, part):
    keys = jax.random.split(key, 4)
    position = jnp.arange(FF, dtype=jnp.float32)
    column_scale = 10.0 ** jax.random.uniform(keys[0], (FF,), jnp.float32) * 3.0 ** (position / FF) / 4.0
    row_scale = 10.0 ** jax.random.uniform(keys[1], (GROUPS, TOK_GROUP, 1), jnp.float32) / 4.0
    owner = jax.random.permutation(keys[2], SHARDS)
    token_block = jnp.arange(TOK_GROUP) // TOK_DEV
    unit_block = jnp.arange(FF) // (FF // SHARDS)
    spike = jnp.where(owner[token_block][:, None] == unit_block[None, :], 3.0, 1.0)
    shape = (GROUPS, TOK_GROUP, FF)
    base = jnp.clip(jax.random.normal(keys[3], shape, jnp.float32), -5.0, 5.0)
    return (base * row_scale * column_scale * spike).astype(jnp.bfloat16)


def draw_upstream(key, part):
    keys = jax.random.split(key, 2)
    column_scale = 10.0 ** jax.random.uniform(keys[0], (D,), jnp.float32) / 3.0
    shape = (GROUPS, TOK_GROUP, D)
    base = jnp.clip(jax.random.normal(keys[1], shape, jnp.float32), -5.0, 5.0)
    return (base * column_scale).astype(jnp.bfloat16)


def steps_of(stream_key, shape, shards, smallest, high):
    gain, own = 1.0, jax.random.fold_in(stream_key, 6)
    for axis_at, parts in shards:
        heights = jnp.exp(jax.random.uniform(jax.random.fold_in(own, axis_at), (parts,), jnp.float32, smallest / len(shards), high / len(shards)))
        gain = gain * jnp.repeat(heights, shape[axis_at] // parts).reshape([-1 if axis == axis_at else 1 for axis in range(len(shape))])
    return gain


def scatter_about(own_key, dims, scale, bound, cuts=(), held_as=jnp.bfloat16):
    level = steps_of(own_key, dims, cuts, -0.22, 0.18) if cuts else 1.0
    result = jax.random.normal(own_key, dims, jnp.float32) * scale * level
    return jnp.minimum(jnp.maximum(result, -bound), bound).astype(held_as)


def setup_inputs(seed: int = 0) -> dict:
    splits = jax.random.split(jax.random.key(seed), 6)
    return {
        "step_index": jax.random.randint(splits[0], (1,), 0, 1024).astype(jnp.int32),
        "hidden": draw_hidden(jax.random.fold_in(splits[5], 71), 0),
        "upstream": draw_upstream(jax.random.fold_in(splits[5], 71), 0),
        "numerator": scatter_about(splits[3], (GROUPS, FF, D), 1.0, 6.0, ((0, 4), (1, 8)), jnp.float32),
        "push_weight": jnp.clip(jnp.exp(math.log(2.0) - 1.3862944 * jax.random.uniform(splits[4], (GROUPS,), jnp.float32) ** steps_of(splits[4], (GROUPS,), ((0, 4),), -0.2, 0.2)), 0.5, 2.0),
    }


learning_rate = 0.3
decay_steps = 256.0
clip_ceiling = 1.0
epsilon = 1e-06

def shard_gradient(hidden_rows, upstream_rows):
    hidden_blocks = hidden_rows.reshape(SHARDS, TOK_DEV, FF)
    upstream_blocks = upstream_rows.reshape(SHARDS, TOK_DEV, D)

    def accumulate(running, shard_pair):
        product = jnp.dot(shard_pair[0].astype(jnp.float32).T, shard_pair[1].astype(jnp.float32), preferred_element_type=jnp.float32, precision=lax.Precision.HIGHEST)
        rounded = lax.optimization_barrier(product.astype(jnp.bfloat16))
        return (running + rounded.astype(jnp.float32), None)
    summed, unused = lax.scan(accumulate, jnp.zeros((FF, D), jnp.float32), (hidden_blocks, upstream_blocks))
    return summed

def group_pair(arrays):
    return shard_gradient(arrays[0], arrays[1])

def reference(step_index, hidden, upstream, numerator, push_weight):
    gradient = lax.map(group_pair, (hidden, upstream))
    square_mean = lax.optimization_barrier(jnp.sum(gradient * gradient, axis=(1, 2))) / (FF * D)
    rate = learning_rate / jnp.sqrt(1.0 + step_index[0].astype(jnp.float32) / decay_steps)
    factor = rate * jnp.minimum(1.0, clip_ceiling / jnp.sqrt(square_mean + epsilon))
    pushed = numerator - factor[:, None, None] * gradient
    level_count = GROUPS.bit_length() - 1
    exponent = (step_index[0] % level_count).astype(jnp.int32)
    offset = jnp.left_shift(jnp.int32(1), exponent)
    peer_state = jnp.roll(pushed, offset, axis=0)
    peer_weight = jnp.roll(push_weight, offset, axis=0)
    numerator_next = 0.5 * (pushed + peer_state)
    weight_next = 0.5 * (push_weight + peer_weight)
    params = (numerator_next / weight_next[:, None, None]).astype(jnp.bfloat16)
    return (numerator_next, weight_next, params)
```

```python
import functools

import jax
import jax.numpy as jnp
from jax import lax
from jax.experimental import pallas as pl
from jax.experimental.pallas import tpu as pltpu
from jax.sharding import PartitionSpec as P

learning_rate = 0.3
decay_steps = 256.0
clip_ceiling = 1.0
epsilon = 1e-06
LANES = 128
LINKED = jnp.bfloat16
MESH = pl.DeviceIdType.MESH
FAR_FIRST_TILES = 3
NEAR_FIRST_TILES = (4, 4, 3, 2, 1, 1)


def wide(x):
    return x.astype(jnp.float32)


def cuts(width):
    tiles = width // LANES
    sizes = (FAR_FIRST_TILES,) + NEAR_FIRST_TILES
    if tiles != sum(sizes) or width % LANES:
        half = (tiles // 2) * LANES
        sizes = (half, width - half)
    else:
        sizes = tuple(s * LANES for s in sizes)
    starts = [sum(sizes[:i]) for i in range(len(sizes))]
    return list(zip(starts, sizes))


def step_of_rows(rows):
    for step in (64, 48, 32, 16):
        if rows % step == 0:
            return step
    return rows


def kernel(plan, partial, state, weight, grad, totals, *refs):
    groups, far, near, rows, pieces, offsets = (
        plan["groups"], plan["far"], plan["near"], plan["rows"], plan["pieces"], plan["offsets"]
    )
    levels, count = len(offsets), far * near
    peer_states, peer_grads = refs[:levels], refs[levels : 2 * levels]
    refs = list(refs[2 * levels :])
    mine = [refs.pop(0) for _ in pieces]
    came = [None] + [refs.pop(0) for _ in pieces[1:]]
    slots = [refs.pop(0) for _ in pieces]
    ready = [refs.pop(0) for _ in pieces]
    turn_out, turn_in, norms, own_total = (refs.pop(0) for _ in range(4))
    (load_sem, near_send, near_recv, up_send, up_recv, down_send, down_recv, turn_sem, state_send, state_recv,
     grad_send, grad_recv, norm_send, norm_recv, total_send, total_recv) = refs

    g, s = lax.axis_index("group"), lax.axis_index("shard")
    z, y = s // near, s % near
    near_peer = (g, z * near + (near - 1 - y))
    above = (g, (s + near) % count)
    below = (g, (s + count - near) % count)
    step_rows = step_of_rows(rows)

    barrier = pltpu.get_barrier_semaphore()
    for d in range(1, count):
        pl.semaphore_signal(barrier, inc=1, device_id=(g, (s + d) % count), device_id_type=MESH)
    for d in range(1, groups):
        pl.semaphore_signal(barrier, inc=1, device_id=((g + d) % groups, s), device_id_type=MESH)
    pl.semaphore_wait(barrier, count - 1 + groups - 1)

    def remote(src, dst, send, recv, device):
        return pltpu.make_async_remote_copy(
            src_ref=src, dst_ref=dst, send_sem=send, recv_sem=recv, device_id=device, device_id_type=MESH
        )

    def near_copy(c):
        start, size = pieces[c]
        return remote(
            partial.at[:, near - 1 - y, :, pl.ds(start, size)], came[c], near_send.at[c], near_recv.at[c], near_peer
        )

    def load_copy(c):
        start, size = pieces[c]
        at = partial.at[:, :, :, pl.ds(start, size)] if c == 0 else partial.at[:, y, :, pl.ds(start, size)]
        return pltpu.make_async_copy(at, mine[c], load_sem.at[c])

    def up_copy(c, t, b):
        return remote(slots[c].at[b], slots[c].at[b], up_send.at[c, t], up_recv.at[c, t], above)

    def down_copy(c, t, b):
        to = far if t == far - 2 else b
        return remote(slots[c].at[b], slots[c].at[to], down_send.at[c, t], down_recv.at[c, t], below)

    def state_copy(l):
        return remote(
            state, peer_states[l], state_send.at[l], state_recv.at[l], ((g + offsets[l]) % groups, s)
        )

    def grad_copy(c, l):
        start, size = pieces[c]
        return remote(
            ready[c],
            peer_grads[l].at[:, pl.ds(start, size)],
            grad_send.at[c, l],
            grad_recv.at[c, l],
            ((g + offsets[l]) % groups, s),
        )

    def each_rows(body):
        def once(i, carry):
            body(pl.ds(pl.multiple_of(i * step_rows, step_rows), step_rows))
            return carry

        lax.fori_loop(0, rows // step_rows, once, 0)

    def term(c, b, r, half):
        if c == 0:
            return wide(mine[0][b, half, r, :])
        return wide(mine[c][b, r, :]) + wide(came[c][b, r, :])

    def slot(c, b, r, half):
        return slots[c][b, half, r, :] if c == 0 else slots[c][b, r, :]

    def store_slot(c, b, r, half, value):
        if c == 0:
            slots[c][b, half, r, :] = value.astype(LINKED)
        else:
            slots[c][b, r, :] = value.astype(LINKED)

    def halves(c):
        return range(near) if c == 0 else range(1)

    def fill(c, b, add):
        for half in halves(c):
            def body(r):
                value = term(c, b, r, half)
                if add:
                    value = value + wide(slot(c, b, r, half))
                store_slot(c, b, r, half, value)

            each_rows(body)

    def line_step(c, t):
        up_b = far - 1 - t + z
        down_b = t - (far - 1) + z

        @pl.when(z == 0)
        def _():
            fill(c, up_b, False)
            up_copy(c, t, up_b).start()

        if t > 0:
            @pl.when((z > 0) & (z <= t) & (z < far - 1))
            def _():
                up_copy(c, t - 1, up_b).wait_recv()
                fill(c, up_b, True)
                up_copy(c, t, up_b).start()

        @pl.when(z == far - 1)
        def _():
            fill(c, down_b, False)
            down_copy(c, t, down_b).start()

        if t > 0:
            @pl.when((z < far - 1) & (z >= far - 1 - t) & (z > 0))
            def _():
                down_copy(c, t - 1, down_b).wait_recv()
                fill(c, down_b, True)
                down_copy(c, t, down_b).start()

    def own_value(c, r, half):
        value = term(c, z, r, half)
        below_term = jnp.where(z > 0, wide(slot(c, z, r, half)), 0.0)
        above_term = jnp.where(z < far - 1, wide(slot(c, far, r, half)), 0.0)
        return value + below_term + above_term

    def wait_own(c):
        @pl.when(z > 0)
        def _():
            up_copy(c, far - 2, z).wait_recv()

        @pl.when(z < far - 1)
        def _():
            down_copy(c, far - 2, far).wait_recv()

    def settle(c, r, value):
        start, size = pieces[c]
        grad[r, pl.ds(start, size)] = value
        ready[c][r, :] = value.astype(LINKED)
        square = value * value
        total = jnp.zeros((8, LANES), jnp.float32)
        for i in range(0, step_rows, 8):
            for j in range(0, size, LANES):
                total = total + square[i : i + 8, j : j + LANES]
        own_total[0] = own_total[0] + total

    def finish(c):
        wait_own(c)
        if c == 0:
            def put(r):
                start, size = pieces[0]
                grad[r, pl.ds(start, size)] = own_value(0, r, y)
                turn_out[r, :] = own_value(0, r, near - 1 - y).astype(LINKED)

            each_rows(put)
            remote(turn_out, turn_in, turn_sem.at[0], turn_sem.at[1], near_peer).start()
            return
        each_rows(lambda r: settle(c, r, own_value(c, r, 0)))
        for l in range(levels):
            grad_copy(c, l).start()

    def finish_turn():
        start, size = pieces[0]
        remote(turn_out, turn_in, turn_sem.at[0], turn_sem.at[1], near_peer).wait()
        each_rows(lambda r: settle(0, r, grad[r, pl.ds(start, size)] + wide(turn_in[r, :])))
        for l in range(levels):
            grad_copy(0, l).start()

    last = len(pieces) - 1
    load_copy(0).start()
    for c in range(1, min(3, last + 1)):
        near_copy(c).start()
    for l in range(levels):
        state_copy(l).start()
    for c in range(1, last + 1):
        load_copy(c).start()
    own_total[0] = jnp.zeros((8, LANES), jnp.float32)
    own_total[1] = weight[...]

    load_copy(0).wait()
    for t in range(far - 1):
        line_step(0, t)
    for c in range(1, last + 1):
        near_copy(c).wait()
        if c + 2 <= last:
            near_copy(c + 2).start()
        load_copy(c).wait()
        line_step(c, 0)
        finish(c - 1)
        if c == 3 or (c == last and last < 3):
            finish_turn()
        for t in range(1, far - 1):
            line_step(c, t)
    finish(last)

    norms[s] = own_total[0]
    for d in range(1, count):
        remote(norms.at[s], norms.at[s], norm_send.at[d], norm_recv.at[d], (g, (s + d) % count)).start()
    for d in range(1, count):
        remote(norms.at[s], norms.at[(s + count - d) % count], norm_send.at[d], norm_recv.at[d], (g, (s + d) % count)).wait_recv()
    total = norms[0]
    for d in range(1, count):
        total = total + norms[d]
    own_total[0] = total
    totals[0] = own_total[...]

    def total_copy(l):
        return remote(
            own_total, totals.at[l + 1], total_send.at[l], total_recv.at[l], ((g + offsets[l]) % groups, s)
        )

    for l in range(levels):
        total_copy(l).start()
    for d in range(1, count):
        remote(norms.at[s], norms.at[s], norm_send.at[d], norm_recv.at[d], (g, (s + d) % count)).wait_send()
    for c in range(last + 1):
        for t in range(far - 1):
            @pl.when((z <= t) & (z < far - 1))
            def _():
                up_copy(c, t, far - 1 - t + z).wait_send()

            @pl.when((z >= far - 1 - t) & (z > 0))
            def _():
                down_copy(c, t, t - (far - 1) + z).wait_send()

        for l in range(levels):
            grad_copy(c, l).wait()
    for l in range(levels):
        state_copy(l).wait()
        total_copy(l).wait()


def reduced(partial, state, weight, plan):
    far, near, rows, pieces = plan["far"], plan["near"], plan["rows"], plan["pieces"]
    levels, count, width = len(plan["offsets"]), far * near, state.shape[1]
    anywhere, vmem = pl.BlockSpec(memory_space=pl.ANY), pl.BlockSpec(memory_space=pltpu.VMEM)
    first = pieces[0][1]
    scratch = [pltpu.VMEM((far, near, rows, first), LINKED)]
    scratch += [pltpu.VMEM((far, rows, size), LINKED) for _, size in pieces[1:]]
    scratch += [pltpu.VMEM((far, rows, size), LINKED) for _, size in pieces[1:]]
    scratch += [pltpu.VMEM((far + 1, near, rows, first), LINKED)]
    scratch += [pltpu.VMEM((far + 1, rows, size), LINKED) for _, size in pieces[1:]]
    scratch += [pltpu.VMEM((rows, size), LINKED) for _, size in pieces]
    scratch += [pltpu.VMEM((rows, first), LINKED)] * 2
    scratch += [pltpu.VMEM((count, 8, LANES), jnp.float32), pltpu.VMEM((2, 8, LANES), jnp.float32)]
    n = len(pieces)
    dma = pltpu.SemaphoreType.DMA
    scratch += [dma((n,))] * 3 + [dma((n, far - 1))] * 4 + [dma((2,))] + [dma((levels,))] * 2
    scratch += [dma((n, levels))] * 2 + [dma((count,))] * 2 + [dma((levels,))] * 2
    linked = jax.ShapeDtypeStruct((rows, width), LINKED)
    return pl.pallas_call(
        functools.partial(kernel, plan),
        out_shape=[
            jax.ShapeDtypeStruct((rows, width), jnp.float32),
            jax.ShapeDtypeStruct((levels + 1, 2, 8, LANES), jnp.float32),
        ]
        + [linked] * (2 * levels),
        in_specs=[anywhere, anywhere, vmem],
        out_specs=[vmem, vmem] + [anywhere] * (2 * levels),
        scratch_shapes=scratch,
        compiler_params=pltpu.CompilerParams(
            collective_id=0, has_side_effects=True, vmem_limit_bytes=60 * 1024 * 1024
        ),
    )(partial, state, weight)


def shards(step_index, hidden, upstream, numerator, push_weight):
    own_state = numerator[0]
    groups = lax.axis_size("group")
    count = lax.axis_size("shard")
    near = 2
    level_count = groups.bit_length() - 1
    offset_bit = step_index[0] % level_count
    rate = learning_rate / jnp.sqrt(1.0 + step_index[0].astype(jnp.float32) / decay_steps)
    rows, width = own_state.shape
    entry_count = rows * count * width
    plan = {
        "groups": groups,
        "far": count // near,
        "near": near,
        "rows": rows,
        "pieces": cuts(width),
        "offsets": tuple(1 << bit for bit in range(level_count)),
    }
    partial = lax.dot_general(
        hidden[0], upstream[0], (((0,), (0,)), ((), ())), preferred_element_type=jnp.float32
    ).astype(LINKED)
    weight = jnp.broadcast_to(push_weight[0], (8, LANES))
    gradient, totals, *peers = reduced(
        partial.reshape(count // near, near, rows, width), own_state.astype(LINKED), weight, plan
    )
    squares = jnp.sum(totals[:, 0], axis=(1, 2))
    factors = rate * jnp.minimum(1.0, clip_ceiling / jnp.sqrt(squares / entry_count + epsilon))

    def chosen(values):
        got = values[0]
        for bit in range(1, level_count):
            got = jnp.where(offset_bit == bit, values[bit], got)
        return got

    peer_state = wide(chosen(peers[:level_count]))
    peer_gradient = wide(chosen(peers[level_count:]))
    peer_factor = chosen([factors[bit + 1] for bit in range(level_count)])
    peer_weight = chosen([totals[bit + 1, 1, 0, 0] for bit in range(level_count)])
    mixed_state = 0.5 * (own_state - factors[0] * gradient + (peer_state - peer_factor * peer_gradient))
    weight_next = 0.5 * (push_weight + peer_weight)
    new_params = (mixed_state / weight_next[0]).astype(jnp.bfloat16)
    return (mixed_state[None], weight_next, new_params[None])


def solution(mesh):
    placed = (
        P(),
        P("group", "shard", None),
        P("group", "shard", None),
        P("group", "shard", None),
        P("group"),
    )
    return jax.shard_map(
        shards,
        mesh=mesh,
        in_specs=placed,
        out_specs=(P("group", "shard", None), P("group"), P("group", "shard", None)),
        check_vma=False,
    )
```
